32 devices in a mesh: win: 8 (over z, y), tile: 4 (over x, core).
Axes of the slice: x: 2, y: 2, z: 4, core: 2. Of those that a mesh axis runs over, the one named last changes fastest.
Arguments:
- right_side: float32 [8, 2, 128, 1024], P('win', None, 'tile'), may hold values from -64 to 64
- error_weight: float32 [8, 2, 128, 1024], P('win', None, 'tile'), may hold values from 0.5 to 4
- coeffs: float32 [4, 8, 2, 128, 1024], P(None, 'win', None, 'tile'), may hold values from 0.1 to 0.4
- obs_block: int32 [8, 128], P('win', 'tile'), may hold values from 0 to 511
- obs_pos: int32 [8, 128, 128], P('win', 'tile'), may hold values from 0 to 127
- obs_weight: float32 [8, 128, 128], P('win', 'tile'), may hold values from 0.5 to 4
Outputs:
- solution_field: float32 [8, 2, 128, 1024], P('win', None, 'tile')
- residual: float32 [8, 2, 128, 1024], P('win', None, 'tile')
The draws below stay inside these ranges and needn't reach their ends.
All inputs are finite; a program needn't handle non-finite values.
Results may differ from the reference program's by a relative error of at most 0.0001.
Values sent between devices are 32-bit elements; how exact they have to be, the bound alone decides.
A program may use at most 64 MiB of HBM per device.

```python
import math
import jax
import jax.numpy as jnp

LEV = 2
TY = 32
NX = 1024
NBLK = 32
OBSW = 128
ITERS = 3
NWIN = 8
NY = 128
BROWS = 512
N_TILE = 4


def draw_right_side(key, part):
    gaussian = jax.random.normal(jax.random.fold_in(key, 11), (NWIN, LEV, NY, NX), jnp.float32)
    gaussian = jnp.clip(gaussian, -6.0, 6.0)
    growth = 1.0 + 2.0 * jnp.arange(NWIN, dtype=jnp.float32) / max(NWIN - 1, 1)
    growth = growth.reshape(NWIN, 1, 1, 1)
    return growth * gaussian


def place_ends(entries, own_key, low, top_value):
    longest = entries.shape.index(max(entries.shape))
    spots = []
    for shift in (0, 1):
        where = [jax.random.randint(jax.random.fold_in(own_key, axis), (), 0, length) for axis, length in enumerate(entries.shape)]
        where[longest] = (where[longest] + shift) % entries.shape[longest]
        spots.append(tuple(where))
    return entries.at[spots[0]].set(low).at[spots[1]].set(top_value)


def block_levels(key, extent, pieces, smallest, largest):
    def one(axis_at, shards_of):
        heights = jax.random.uniform(jax.random.fold_in(jax.random.fold_in(key, 6), axis_at), (shards_of,), jnp.float32, smallest / len(pieces), largest / len(pieces))
        return jnp.repeat(jnp.exp(heights), extent[axis_at] // shards_of).reshape((-1,) + (1,) * (len(extent) - axis_at - 1))

    level = one(*pieces[0])
    for cut in pieces[1:]:
        level = level * one(*cut)
    return level


def setup_inputs(seed: int = 0) -> dict:
    seeds = jax.random.split(jax.random.key(seed), 7)
    right_side = draw_right_side(jax.random.fold_in(seeds[6], 71), 0)
    error_weight = jnp.clip(jnp.exp(math.log(4.0) - 2.0794415 * jax.random.uniform(seeds[1], (NWIN, LEV, NY, NX), jnp.float32) ** block_levels(seeds[1], (NWIN, LEV, NY, NX), ((0, 8), (2, 4)), -0.2, 0.2)), 0.5, 4.0)
    coeffs = jnp.clip(0.1 + 0.3 * jax.random.uniform(seeds[2], (4, NWIN, LEV, NY, NX), jnp.float32) ** block_levels(seeds[2], (4, NWIN, LEV, NY, NX), ((1, 8), (3, 4)), -0.2, 0.2), 0.1, 0.4)
    obs_block = place_ends(jax.random.randint(seeds[3], (NWIN, N_TILE * NBLK), 0, BROWS), jax.random.fold_in(seeds[3], 1), 0, BROWS - 1).astype(jnp.int32)
    obs_pos = place_ends(jax.random.randint(seeds[4], (NWIN, N_TILE * NBLK, OBSW), 0, OBSW), jax.random.fold_in(seeds[4], 1), 0, OBSW - 1).astype(jnp.int32)
    obs_weight = jnp.clip(jnp.exp(math.log(4.0) - 2.0794415 * jax.random.uniform(seeds[5], (NWIN, N_TILE * NBLK, OBSW), jnp.float32) ** block_levels(seeds[5], (NWIN, N_TILE * NBLK, OBSW), ((0, 8), (1, 4)), -0.2, 0.2)), 0.5, 4.0)
    return {"right_side": right_side, "error_weight": error_weight, "coeffs": coeffs, "obs_block": obs_block, "obs_pos": obs_pos, "obs_weight": obs_weight}


def model_step(state, coeffs):
    padded = jnp.pad(state, ((0, 0), (0, 0), (1, 1), (0, 0)))
    north_south = padded[:, :, 2:, :] + padded[:, :, :-2, :]
    return (coeffs[0] * state + coeffs[1] * north_south
            + coeffs[2] * jnp.roll(state, -1, axis=3) + coeffs[3] * jnp.roll(state, 1, axis=3))


def model_adjoint(state, coeffs):
    spread = jnp.pad(coeffs[1] * state, ((0, 0), (0, 0), (1, 1), (0, 0)))
    north_south = spread[:, :, 2:, :] + spread[:, :, :-2, :]
    return (coeffs[0] * state + north_south
            + jnp.roll(coeffs[2] * state, 1, axis=3) + jnp.roll(coeffs[3] * state, -1, axis=3))


def observe(state, obs_block, obs_pos, obs_weight):
    windows = state.shape[0]
    cell_count = LEV * TY * NX
    blocks = state.reshape(windows, LEV, N_TILE, TY, NX).transpose(0, 2, 1, 3, 4).reshape(windows, N_TILE, cell_count)
    flat_index = (obs_block.reshape(windows, N_TILE, NBLK, 1).astype(jnp.int32) * OBSW
                  + obs_pos.reshape(windows, N_TILE, NBLK, OBSW).astype(jnp.int32))
    flat_index = flat_index.reshape(windows, N_TILE, NBLK * OBSW).astype(jnp.int32)
    observed = jnp.take_along_axis(blocks, flat_index, axis=2)
    weighted = observed * obs_weight.reshape(windows, N_TILE, NBLK * OBSW)

    def place(index_row, value_row):
        return jnp.zeros((cell_count,), jnp.float32).at[index_row].add(value_row)

    spread = jax.vmap(jax.vmap(place))(flat_index, weighted)
    return spread.reshape(windows, N_TILE, LEV, TY, NX).transpose(0, 2, 1, 3, 4).reshape(windows, LEV, NY, NX)


def reference(right_side, error_weight, coeffs, obs_block, obs_pos, obs_weight):
    def hessian(state):
        propagated = model_step(state, coeffs)
        before = jnp.concatenate([jnp.zeros_like(propagated[:1]), propagated[:-1]], axis=0)
        weighted = error_weight * (state - before)
        following = jnp.concatenate([weighted[1:], jnp.zeros_like(weighted[:1])], axis=0)
        return weighted - model_adjoint(following, coeffs) + observe(state, obs_block, obs_pos, obs_weight)

    solution_field = jnp.zeros_like(right_side)
    residual = right_side
    direction = right_side
    norm_now = jnp.sum(residual * residual)
    for iteration in range(ITERS):
        product_vec = hessian(direction)
        step_length = norm_now / jnp.sum(direction * product_vec)
        solution_field = solution_field + step_length * direction
        residual = residual - step_length * product_vec
        norm_next = jnp.sum(residual * residual)
        direction = residual + (norm_next / norm_now) * direction
        norm_now = norm_next
    return solution_field, residual
```

```python
import functools

import jax
import jax.numpy as jnp
from jax import lax
from jax.experimental import pallas as pl
from jax.experimental.pallas import tpu as pltpu
from jax.sharding import PartitionSpec as P

ITERS = 3
EDGE = 8


def kernel(wins, tiles, rhs, err, cof, oblk, opos, owgt, x_out, r_out,
           v, y, w, wn, c, d, ob, u, ui, vn, z, eo, ei, go, gi, rt, home, part, red,
           x_sem, xs_sem, l_sem, h_send, h_recv, b_send, b_recv, g_send, g_recv,
           rt_send, rt_recv, rd_send, rd_recv, wn_send, wn_recv):
    me_w = lax.axis_index("win")
    me_t = lax.axis_index("tile")
    lev = lax.rem(me_w, 2)
    other = 1 - lev
    mate = me_w + 1 - 2 * lev
    has_next = me_w + 2 < wins
    has_prev = me_w >= 2
    has_north = me_t > 0
    has_south = me_t < tiles - 1
    rows, cols = v.shape[2], v.shape[3]
    count = wins * tiles
    me = me_w * tiles + me_t
    width = opos.shape[2]
    nblk = opos.shape[1]

    def remote(src, dst, ssem, rsem, win, tile):
        return pltpu.make_async_remote_copy(
            src_ref=src, dst_ref=dst, send_sem=ssem, recv_sem=rsem,
            device_id=(win, tile), device_id_type=pl.DeviceIdType.MESH)

    swaps = [
        remote(rhs.at[0, other], v.at[0, lev], xs_sem.at[0], x_sem.at[0], mate, me_t),
        remote(err.at[0, other], w.at[lev], xs_sem.at[1], x_sem.at[1], mate, me_t),
    ] + [
        remote(cof.at[k, 0, other], c.at[k, lev], xs_sem.at[2 + k], x_sem.at[2 + k], mate, me_t)
        for k in range(4)
    ]
    for s in swaps:
        s.start()
    locs = [
        pltpu.make_async_copy(rhs.at[0, lev], v.at[0, lev], l_sem.at[0]),
        pltpu.make_async_copy(err.at[0, lev], w.at[lev], l_sem.at[1]),
        pltpu.make_async_copy(rhs.at[0, other], home, l_sem.at[2]),
    ] + [
        pltpu.make_async_copy(cof.at[k, 0, lev], c.at[k, lev], l_sem.at[3 + k]) for k in range(4)
    ]
    for s in locs:
        s.start()

    @pl.when(jnp.logical_not(has_north))
    def _():
        for it in range(ITERS):
            ei[it, 0] = jnp.zeros(ei.shape[2:], jnp.float32)
            gi[it, 0] = jnp.zeros(gi.shape[2:], jnp.float32)

    @pl.when(jnp.logical_not(has_south))
    def _():
        for it in range(ITERS):
            ei[it, 1] = jnp.zeros(ei.shape[2:], jnp.float32)
            gi[it, 1] = jnp.zeros(gi.shape[2:], jnp.float32)

    @pl.when(jnp.logical_not(has_prev))
    def _():
        for it in range(ITERS):
            ui[it] = jnp.zeros(ui.shape[1:], jnp.float32)

    @pl.when(jnp.logical_not(has_next))
    def _():
        wn[...] = jnp.zeros(wn.shape, jnp.float32)
        for it in range(ITERS):
            vn[it] = jnp.zeros(vn.shape[1:], jnp.float32)

    cell = lax.broadcasted_iota(jnp.int32, (width, width), 0)
    ones = jnp.ones((8, width), jnp.float32)
    ob[lev, nblk:, :] = jnp.zeros((8, width), jnp.float32)

    def per_block(b, carry):
        hit = jnp.where(cell == opos[0, pl.ds(b, 1), :], owgt[0, pl.ds(b, 1), :], 0.0)
        total = lax.dot_general(ones, hit, (((1,), (1,)), ((), ())),
                                precision=lax.Precision.HIGHEST,
                                preferred_element_type=jnp.float32)
        ob[lev, pl.ds(b, 1), :] = total[0:1]
        return carry

    lax.fori_loop(0, nblk, per_block, 0)
    ob[lev, nblk:nblk + 1, 0:nblk] = oblk[...].astype(jnp.float32)
    ob_copy = remote(ob.at[lev], ob.at[lev], xs_sem.at[6], x_sem.at[6], mate, me_t)
    ob_copy.start()

    def arrived(k):
        return [
            lambda: remote(rhs.at[0, other], v.at[0, other], xs_sem.at[0], x_sem.at[0], mate, me_t),
            lambda: remote(err.at[0, other], w.at[other], xs_sem.at[1], x_sem.at[1], mate, me_t),
        ][k]()

    pieces = ((0, EDGE), (rows - EDGE, EDGE), (EDGE, rows - 2 * EDGE))

    def edge_copies(out, into, ssem, rsem, it):
        north = remote(out.at[it, 0], into.at[it, 1], ssem.at[it, 0], rsem.at[it, 1],
                       me_w, me_t - 1)
        south = remote(out.at[it, 1], into.at[it, 0], ssem.at[it, 1], rsem.at[it, 0],
                       me_w, me_t + 1)
        return north, south

    def edges_start(out, into, ssem, rsem, it):
        north, south = edge_copies(out, into, ssem, rsem, it)
        pl.when(has_north)(north.start)
        pl.when(has_south)(south.start)

    def edges_wait_recv(out, into, ssem, rsem, it):
        north, south = edge_copies(out, into, ssem, rsem, it)
        pl.when(has_north)(south.wait_recv)
        pl.when(has_south)(north.wait_recv)

    def edges_wait_send(out, into, ssem, rsem, it):
        north, south = edge_copies(out, into, ssem, rsem, it)
        pl.when(has_north)(north.wait_send)
        pl.when(has_south)(south.wait_send)

    def back_copy(it, k):
        lo, n = pieces[k]
        return remote(v.at[it, 0, pl.ds(lo, n)], vn.at[it, pl.ds(lo, n)],
                      b_send.at[0, it, k], b_recv.at[0, it, k], me_w - 2, me_t)

    def forth_copy(it, k):
        lo, n = pieces[k]
        return remote(u.at[1, pl.ds(lo, n)], ui.at[it, pl.ds(lo, n)],
                      b_send.at[1, it, k], b_recv.at[1, it, k], me_w + 2, me_t)

    def ret_copy(it):
        return remote(y.at[it, other], rt.at[it], rt_send.at[it], rt_recv.at[it], mate, me_t)

    row = lax.broadcasted_iota(jnp.int32, (rows, cols), 0)

    def above(a):
        return jnp.where(row == 0, 0.0, pltpu.roll(a, 1, 0))

    def below(a):
        return jnp.where(row == rows - 1, 0.0, pltpu.roll(a, rows - 1, 0))

    def east(a):
        return pltpu.roll(a, cols - 1, 1)

    def west(a):
        return pltpu.roll(a, 1, 1)

    last = rows - 1
    wn_copy = remote(w.at[0], wn, wn_send, wn_recv, me_w - 2, me_t)

    def product(it):
        for i in range(2):
            eo[it, 0, i:i + 1] = v[it, i, 0:1]
            eo[it, 1, i:i + 1] = v[it, i, last:last + 1]
        edges_start(eo, ei, h_send, h_recv, it)

        @pl.when(has_prev)
        def _():
            for k in range(3):
                back_copy(it, k).start()

        if it == 0:
            locs[1].wait()
            arrived(1).wait_recv()
            pl.when(has_prev)(wn_copy.start)
            for k in range(4):
                locs[3 + k].wait()
                swaps[2 + k].wait_recv()
        else:
            @pl.when(has_next)
            def _():
                for k in range(3):
                    forth_copy(it - 1, k).wait_send()

        for i in (1, 0):
            a = v[it, i]
            u[i] = (c[0, i] * a + c[1, i] * (above(a) + below(a))
                    + c[2, i] * east(a) + c[3, i] * west(a))
            if i == 1:
                pl.when(has_next)(forth_copy(it, 2).start)
        edges_wait_recv(eo, ei, h_send, h_recv, it)
        for i in (1, 0):
            u[i, 0:1] = u[i, 0:1] + c[1, i, 0:1] * ei[it, 0, i:i + 1]
            u[i, last:last + 1] = u[i, last:last + 1] + c[1, i, last:last + 1] * ei[it, 1, i:i + 1]

        @pl.when(has_next)
        def _():
            forth_copy(it, 0).start()
            forth_copy(it, 1).start()
            if it == 0:
                wn_copy.wait_recv()
            back_copy(it, 0).wait_recv()
            back_copy(it, 1).wait_recv()

        for side, at in ((0, 0), (1, last)):
            here = slice(at, at + 1)
            go[it, side, 0:1] = c[1, 0, here] * (w[1, here] * (v[it, 1, here] - u[0, here]))
            go[it, side, 1:2] = c[1, 1, here] * (wn[here] * (vn[it, here] - u[1, here]))
        edges_start(go, gi, g_send, g_recv, it)

        def adjoint(i, q):
            g = c[1, i] * q
            return (c[0, i] * q + (above(g) + below(g)) + west(c[2, i] * q) + east(c[3, i] * q))

        z[...] = w[1] * (v[it, 1] - u[0])
        y[it, 0] = d[0] * v[it, 0] - adjoint(0, z[...])
        pl.when(has_next)(back_copy(it, 2).wait_recv)
        y[it, 1] = (z[...] + d[1] * v[it, 1]) - adjoint(1, wn[...] * (vn[it] - u[1]))

        @pl.when(has_prev)
        def _():
            for k in range(3):
                forth_copy(it, k).wait_recv()

        y[it, 0] = y[it, 0] + w[0] * (v[it, 0] - ui[it])
        edges_wait_recv(go, gi, g_send, g_recv, it)
        for i in range(2):
            y[it, i, 0:1] = y[it, i, 0:1] - gi[it, 0, i:i + 1]
            y[it, i, last:last + 1] = y[it, i, last:last + 1] - gi[it, 1, i:i + 1]
        ret_copy(it).start()

    def folded(a):
        return jnp.sum(jnp.sum(a, axis=0).reshape(-1, 128), axis=0, keepdims=True)

    def lanes(pair):
        a = jnp.sum(pair[0] + pair[1], axis=0, keepdims=True)
        total = a[:, 0:128]
        for k in range(1, cols // 128):
            total = total + a[:, k * 128:(k + 1) * 128]
        return total

    def reduce_start(it, r, aw):
        part[it, 0:1] = lanes(r * r)
        part[it, 1:2] = lanes(r * aw)

        def send(o, carry):
            to = lax.rem(me + o, count)
            remote(part.at[it], red.at[it, me], rd_send.at[it], rd_recv.at[it],
                   to // tiles, lax.rem(to, tiles)).start()
            return carry

        lax.fori_loop(1, count, send, 0)
        red[it, me] = part[it]

    def reduce_end(it):
        most = red.at[it, pl.ds(0, count - 1)]
        pltpu.make_async_copy(most, most, rd_recv.at[it]).wait()
        total = jnp.sum(red[it], axis=0)
        both = jnp.sum(total, axis=1, keepdims=True)
        return both[0:1], both[1:2]

    locs[0].wait()
    arrived(0).wait_recv()

    def diagonal():
        remote(ob.at[lev], ob.at[other], xs_sem.at[6], x_sem.at[6], mate, me_t).wait_recv()
        per_row = cols // width
        base = lev * (rows * per_row)
        spot = lax.broadcasted_iota(jnp.int32, (rows, nblk), 0) * per_row + base
        for i in range(2):
            who = ob[i, nblk:nblk + 1, 0:nblk]
            sums = ob[i, 0:nblk, :]
            for k in range(per_row):
                hot = jnp.where((spot + k).astype(jnp.float32) == who, 1.0, 0.0)
                d[i, :, k * width:(k + 1) * width] = jnp.dot(
                    hot, sums, precision=lax.Precision.HIGHEST,
                    preferred_element_type=jnp.float32)

    diagonal()

    product(0)
    v[1] = y[0]
    reduce_start(0, v[0], y[0])
    product(1)
    g0, d0 = reduce_end(0)
    a0 = g0 / d0
    v[2] = y[0] - a0 * y[1]
    reduce_start(1, v[0] - a0 * y[0], v[2])
    product(2)
    g1, d1 = reduce_end(1)
    b1 = g1 / g0
    a1 = g1 / (d1 - b1 * g1 / a0)

    def second(r0, w0, n0, n1):
        r1 = r0 - a0 * w0
        w1 = w0 - a0 * n0
        s1 = w1 + b1 * w0
        r2 = r1 - a1 * s1
        w2 = w1 - a1 * (n1 + b1 * n0)
        return r1, s1, r2, w2

    _, _, r2, w2 = second(v[0], y[0], y[1], y[2])
    reduce_start(2, r2, w2)

    locs[2].wait()
    for it in range(ITERS):
        ret_copy(it).wait_recv()
    g2, d2 = reduce_end(2)
    b2 = g2 / g1
    a2 = g2 / (d2 - b2 * g2 / a1)

    def finish(level, r0, w0, n0, n1):
        r1, s1, r2, w2 = second(r0, w0, n0, n1)
        p1 = r1 + b1 * r0
        x_out[0, level] = (a0 * r0 + a1 * p1) + a2 * (r2 + b2 * p1)
        r_out[0, level] = r2 - a2 * (w2 + b2 * s1)

    finish(lev, v[0, lev], y[0, lev], y[1, lev], y[2, lev])
    finish(other, home[...], rt[0], rt[1], rt[2])

    for s in swaps:
        s.wait_send()
    ob_copy.wait_send()
    pl.when(has_prev)(wn_copy.wait_send)
    for it in range(ITERS):
        edges_wait_send(eo, ei, h_send, h_recv, it)
        edges_wait_send(go, gi, g_send, g_recv, it)
        ret_copy(it).wait_send()
        most = red.at[it, pl.ds(0, count - 1)]
        pltpu.make_async_copy(most, most, rd_send.at[it]).wait()

        @pl.when(has_prev)
        def _():
            for k in range(3):
                back_copy(it, k).wait_send()

    @pl.when(has_next)
    def _():
        for k in range(3):
            forth_copy(ITERS - 1, k).wait_send()


def on_device(wins, tiles, right_side, error_weight, coeffs, obs_block, obs_pos, obs_weight):
    _, levels, rows, cols = right_side.shape
    nblk, width = obs_pos.shape[1:]
    f32 = jnp.float32
    vm = functools.partial(pltpu.VMEM, dtype=f32)
    dma = pltpu.SemaphoreType.DMA
    anyspace = pl.BlockSpec(memory_space=pl.ANY)
    vmem = pl.BlockSpec(memory_space=pltpu.VMEM)
    scratch = [
        vm((ITERS, 2, rows, cols)),
        vm((ITERS, 2, rows, cols)),
        vm((2, rows, cols)),
        vm((rows, cols)),
        vm((4, 2, rows, cols)),
        vm((2, rows, cols)),
        vm((2, nblk + 8, width)),
        vm((2, rows, cols)),
        vm((ITERS, rows, cols)),
        vm((ITERS, rows, cols)),
        vm((rows, cols)),
        vm((ITERS, 2, 2, cols)),
        vm((ITERS, 2, 2, cols)),
        vm((ITERS, 2, 2, cols)),
        vm((ITERS, 2, 2, cols)),
        vm((ITERS, rows, cols)),
        vm((rows, cols)),
        vm((ITERS, 2, 128)),
        vm((ITERS, wins * tiles, 2, 128)),
        dma((7,)), dma((7,)), dma((7,)),
        dma((ITERS, 2)), dma((ITERS, 2)),
        dma((2, ITERS, 3)), dma((2, ITERS, 3)),
        dma((ITERS, 2)), dma((ITERS, 2)),
        dma((ITERS,)), dma((ITERS,)),
        dma((ITERS,)), dma((ITERS,)),
        dma, dma,
    ]
    out = jax.ShapeDtypeStruct(right_side.shape, f32)
    return pl.pallas_call(
        functools.partial(kernel, wins, tiles),
        out_shape=(out, out),
        in_specs=[anyspace, anyspace, anyspace, vmem, vmem, vmem],
        out_specs=(vmem, vmem),
        scratch_shapes=scratch,
        compiler_params=pltpu.CompilerParams(has_side_effects=True,
                                             vmem_limit_bytes=48 * 1024 * 1024),
    )(right_side, error_weight, coeffs, obs_block, obs_pos, obs_weight)


def solution(mesh):
    in_specs = (
        P("win", None, "tile", None),
        P("win", None, "tile", None),
        P(None, "win", None, "tile", None),
        P("win", "tile"),
        P("win", "tile", None),
        P("win", "tile", None),
    )
    out_specs = (P("win", None, "tile", None), P("win", None, "tile", None))
    return jax.shard_map(
        functools.partial(on_device, mesh.shape["win"], mesh.shape["tile"]),
        mesh=mesh, in_specs=in_specs, out_specs=out_specs, check_vma=False
    )
```

```python
import functools

import jax
import jax.numpy as jnp
from jax import lax
from jax.experimental import pallas as pl
from jax.experimental.pallas import tpu as pltpu
from jax.sharding import PartitionSpec as P

ITERS = 3
EDGE = 8


def kernel(wins, tiles, rhs, err, cof, oblk_in, opos_in, owgt_in, x_out, r_out,
           obk, ops, owt, v, y, w, wn, c, d, ob, u, ui, vn, z, eo, ei, go, gi, rt, home, part, red,
           x_sem, xs_sem, l_sem, h_send, h_recv, b_send, b_recv, g_send, g_recv,
           rt_send, rt_recv, rd_send, rd_recv, wn_send, wn_recv):
    me_w = lax.axis_index("win")
    me_t = lax.axis_index("tile")
    lev = lax.rem(me_w, 2)
    other = 1 - lev
    mate = me_w + 1 - 2 * lev
    has_next = me_w + 2 < wins
    has_prev = me_w >= 2
    has_north = me_t > 0
    has_south = me_t < tiles - 1
    rows, cols = v.shape[2], v.shape[3]
    oblk, opos, owgt = obk, ops, owt
    count = wins * tiles
    me = me_w * tiles + me_t
    width = opos.shape[2]
    nblk = opos.shape[1]

    def remote(src, dst, ssem, rsem, win, tile):
        return pltpu.make_async_remote_copy(
            src_ref=src, dst_ref=dst, send_sem=ssem, recv_sem=rsem,
            device_id=(win, tile), device_id_type=pl.DeviceIdType.MESH)

    pieces = [(0, EDGE), (rows - EDGE, EDGE)] + [
        (lo, EDGE) for lo in range(EDGE, rows - EDGE, EDGE)]
    many = len(pieces)

    swaps = [
        remote(rhs.at[0, other], v.at[0, lev], xs_sem.at[0], x_sem.at[0], mate, me_t),
        remote(err.at[0, other], w.at[lev], xs_sem.at[1], x_sem.at[1], mate, me_t),
    ] + [
        remote(cof.at[:, 0, other, pl.ds(lo, n)], c.at[:, lev, pl.ds(lo, n)],
               xs_sem.at[3 + k], x_sem.at[3 + k], mate, me_t)
        for k, (lo, n) in enumerate(pieces)
    ]
    for s in swaps:
        s.start()
    locs = [
        pltpu.make_async_copy(oblk_in, obk, l_sem.at[4]),
        pltpu.make_async_copy(opos_in, ops, l_sem.at[5]),
        pltpu.make_async_copy(owgt_in, owt, l_sem.at[6]),
        pltpu.make_async_copy(rhs.at[0, lev], v.at[0, lev], l_sem.at[0]),
        pltpu.make_async_copy(err.at[0, lev], w.at[lev], l_sem.at[1]),
        pltpu.make_async_copy(rhs.at[0, other], home, l_sem.at[2]),
        pltpu.make_async_copy(cof.at[:, 0, lev], c.at[:, lev], l_sem.at[3]),
    ]
    for s in locs:
        s.start()
    locs = locs[3:] + locs[:3]

    @pl.when(jnp.logical_not(has_north))
    def _():
        for it in range(ITERS):
            ei[it, 0] = jnp.zeros(ei.shape[2:], jnp.float32)
            gi[it, 0] = jnp.zeros(gi.shape[2:], jnp.float32)

    @pl.when(jnp.logical_not(has_south))
    def _():
        for it in range(ITERS):
            ei[it, 1] = jnp.zeros(ei.shape[2:], jnp.float32)
            gi[it, 1] = jnp.zeros(gi.shape[2:], jnp.float32)

    @pl.when(jnp.logical_not(has_prev))
    def _():
        for it in range(ITERS):
            ui[it] = jnp.zeros(ui.shape[1:], jnp.float32)

    @pl.when(jnp.logical_not(has_next))
    def _():
        wn[...] = jnp.zeros(wn.shape, jnp.float32)
        for it in range(ITERS):
            vn[it] = jnp.zeros(vn.shape[1:], jnp.float32)

    for s in locs[4:]:
        s.wait()
    cell = lax.broadcasted_iota(jnp.int32, (width, width), 0)
    ones = jnp.ones((8, width), jnp.float32)
    ob[lev, nblk:, :] = jnp.zeros((8, width), jnp.float32)

    def per_block(b, carry):
        hit = jnp.where(cell == opos[0, pl.ds(b, 1), :], owgt[0, pl.ds(b, 1), :], 0.0)
        total = lax.dot_general(ones, hit, (((1,), (1,)), ((), ())),
                                precision=lax.Precision.HIGHEST,
                                preferred_element_type=jnp.float32)
        ob[lev, pl.ds(b, 1), :] = total[0:1]
        return carry

    lax.fori_loop(0, nblk, per_block, 0)
    ob[lev, nblk:nblk + 1, 0:nblk] = oblk[...].astype(jnp.float32)
    ob_copy = remote(ob.at[lev], ob.at[lev], xs_sem.at[2], x_sem.at[2], mate, me_t)
    ob_copy.start()

    states = (v.at[0], y.at[0], v.at[1])

    def arrived(k):
        return [
            lambda: remote(rhs.at[0, other], v.at[0, other], xs_sem.at[0], x_sem.at[0], mate, me_t),
            lambda: remote(err.at[0, other], w.at[other], xs_sem.at[1], x_sem.at[1], mate, me_t),
        ][k]()


    def edge_copies(out, into, ssem, rsem, it):
        north = remote(out.at[it, 0], into.at[it, 1], ssem.at[it, 0], rsem.at[it, 1],
                       me_w, me_t - 1)
        south = remote(out.at[it, 1], into.at[it, 0], ssem.at[it, 1], rsem.at[it, 0],
                       me_w, me_t + 1)
        return north, south

    def edges_start(out, into, ssem, rsem, it):
        north, south = edge_copies(out, into, ssem, rsem, it)
        pl.when(has_north)(north.start)
        pl.when(has_south)(south.start)

    def edges_wait_recv(out, into, ssem, rsem, it):
        north, south = edge_copies(out, into, ssem, rsem, it)
        pl.when(has_north)(south.wait_recv)
        pl.when(has_south)(north.wait_recv)

    def edges_wait_send(out, into, ssem, rsem, it):
        north, south = edge_copies(out, into, ssem, rsem, it)
        pl.when(has_north)(north.wait_send)
        pl.when(has_south)(south.wait_send)

    def back_copy(it, k):
        lo, n = pieces[k]
        return remote(states[it].at[0, pl.ds(lo, n)], vn.at[it, pl.ds(lo, n)],
                      b_send.at[0, it, k], b_recv.at[0, it, k], me_w - 2, me_t)

    def forth_copy(it, k):
        lo, n = pieces[k]
        return remote(u.at[1, pl.ds(lo, n)], ui.at[it, pl.ds(lo, n)],
                      b_send.at[1, it, k], b_recv.at[1, it, k], me_w + 2, me_t)

    def ret_copy(it):
        return remote(y.at[it, other], rt.at[it], rt_send.at[it], rt_recv.at[it], mate, me_t)

    row = lax.broadcasted_iota(jnp.int32, (rows, cols), 0)
    row8 = lax.broadcasted_iota(jnp.int32, (EDGE, cols), 0)

    def above(a):
        return jnp.where(row == 0, 0.0, pltpu.roll(a, 1, 0))

    def below(a):
        return jnp.where(row == rows - 1, 0.0, pltpu.roll(a, rows - 1, 0))

    def east(a):
        return pltpu.roll(a, cols - 1, 1)

    def west(a):
        return pltpu.roll(a, 1, 1)

    last = rows - 1
    wn_copy = remote(w.at[0], wn, wn_send, wn_recv, me_w - 2, me_t)

    def model_piece(it, i, k):
        lo, n = pieces[k]
        src = states[it]
        a = src[i, lo:lo + n]
        top = ei[it, 0, i:i + 1] if lo == 0 else src[i, lo - 1:lo]
        bottom = ei[it, 1, i:i + 1] if lo + n == rows else src[i, lo + n:lo + n + 1]
        sides = (jnp.where(row8 == 0, top, pltpu.roll(a, 1, 0))
                 + jnp.where(row8 == n - 1, bottom, pltpu.roll(a, n - 1, 0)))
        u[i, lo:lo + n] = (c[0, i, lo:lo + n] * a + c[1, i, lo:lo + n] * sides
                           + c[2, i, lo:lo + n] * east(a) + c[3, i, lo:lo + n] * west(a))

    def sends(it):
        src = states[it]
        for i in range(2):
            eo[it, 0, i:i + 1] = src[i, 0:1]
            eo[it, 1, i:i + 1] = src[i, last:last + 1]
        edges_start(eo, ei, h_send, h_recv, it)

        @pl.when(has_prev)
        def _():
            for k in range(many):
                back_copy(it, k).start()

    def product(it, beside):
        src = states[it]
        sends(it)
        beside()
        if it == 0:
            locs[1].wait()
            arrived(1).wait_recv()
            pl.when(has_prev)(wn_copy.start)
            locs[3].wait()
            edges_wait_recv(eo, ei, h_send, h_recv, it)
            for k in range(many):
                swaps[2 + k].wait_recv()
                model_piece(it, 1, k)
                pl.when(has_next)(forth_copy(it, k).start)
                model_piece(it, 0, k)
                if k == 1:
                    adjoint_edges(it)
        else:
            @pl.when(has_next)
            def _():
                for k in range(many):
                    forth_copy(it - 1, k).wait_send()

            for k in range(2, many):
                model_piece(it, 1, k)
                pl.when(has_next)(forth_copy(it, k).start)
            edges_wait_recv(eo, ei, h_send, h_recv, it)
            for k in range(2):
                model_piece(it, 1, k)
                pl.when(has_next)(forth_copy(it, k).start)
            for k in range(2):
                model_piece(it, 0, k)
            adjoint_edges(it)
            for k in range(2, many):
                model_piece(it, 0, k)

        def adjoint(i, q):
            g = c[1, i] * q
            return (c[0, i] * q + (above(g) + below(g)) + west(c[2, i] * q) + east(c[3, i] * q))

        z[...] = w[1] * (src[1] - u[0])
        y[it, 0] = d[0] * src[0] - adjoint(0, z[...])

        @pl.when(has_next)
        def _():
            for k in range(2, many):
                back_copy(it, k).wait_recv()

        y[it, 1] = (z[...] + d[1] * src[1]) - adjoint(1, wn[...] * (vn[it] - u[1]))

        edges_wait_recv(go, gi, g_send, g_recv, it)
        for i in range(2):
            y[it, i, 0:1] = y[it, i, 0:1] - gi[it, 0, i:i + 1]
            y[it, i, last:last + 1] = y[it, i, last:last + 1] - gi[it, 1, i:i + 1]

        @pl.when(has_prev)
        def _():
            for k in range(many):
                forth_copy(it, k).wait_recv()

        y[it, 0] = y[it, 0] + w[0] * (src[0] - ui[it])

    def adjoint_edges(it):
        src = states[it]

        @pl.when(has_next)
        def _():
            if it == 0:
                wn_copy.wait_recv()
            back_copy(it, 0).wait_recv()
            back_copy(it, 1).wait_recv()

        for side, at in ((0, 0), (1, last)):
            here = slice(at, at + 1)
            go[it, side, 0:1] = c[1, 0, here] * (w[1, here] * (src[1, here] - u[0, here]))
            go[it, side, 1:2] = c[1, 1, here] * (wn[here] * (vn[it, here] - u[1, here]))
        edges_start(go, gi, g_send, g_recv, it)

    def lanes(pair):
        a = jnp.sum(pair[0] + pair[1], axis=0, keepdims=True)
        total = a[:, 0:128]
        for k in range(1, cols // 128):
            total = total + a[:, k * 128:(k + 1) * 128]
        return total

    def reduce_start(it, r, aw):
        part[it, 0:1] = lanes(r * r)
        part[it, 1:2] = lanes(r * aw)

        def send(o, carry):
            to = lax.rem(me + o, count)
            remote(part.at[it], red.at[it, me], rd_send.at[it], rd_recv.at[it],
                   to // tiles, lax.rem(to, tiles)).start()
            return carry

        lax.fori_loop(1, count, send, 0)
        red[it, me] = part[it]

    def reduce_end(it):
        most = red.at[it, pl.ds(0, count - 1)]
        pltpu.make_async_copy(most, most, rd_recv.at[it]).wait()
        total = jnp.sum(red[it], axis=0)
        both = jnp.sum(total, axis=1, keepdims=True)
        return both[0:1], both[1:2]

    locs[0].wait()
    arrived(0).wait_recv()

    def diagonal():
        remote(ob.at[lev], ob.at[other], xs_sem.at[2], x_sem.at[2], mate, me_t).wait_recv()
        per_row = cols // width
        base = lev * (rows * per_row)
        spot = lax.broadcasted_iota(jnp.int32, (rows, nblk), 0) * per_row + base
        for i in range(2):
            who = ob[i, nblk:nblk + 1, 0:nblk]
            sums = ob[i, 0:nblk, :]
            for k in range(per_row):
                hot = jnp.where((spot + k).astype(jnp.float32) == who, 1.0, 0.0)
                d[i, :, k * width:(k + 1) * width] = jnp.dot(
                    hot, sums, precision=lax.Precision.HIGHEST,
                    preferred_element_type=jnp.float32)

    product(0, diagonal)

    def first_sums():
        ret_copy(0).start()
        reduce_start(0, v[0], y[0])

    product(1, first_sums)
    g0, d0 = reduce_end(0)
    a0 = g0 / d0
    v[1] = y[0] - a0 * y[1]

    def second_sums():
        ret_copy(1).start()
        reduce_start(1, v[0] - a0 * y[0], v[1])

    product(2, second_sums)
    g1, d1 = reduce_end(1)
    b1 = g1 / g0
    a1 = g1 / (d1 - b1 * g1 / a0)

    def second(r0, w0, n0, n1):
        r1 = r0 - a0 * w0
        w1 = w0 - a0 * n0
        s1 = w1 + b1 * w0
        r2 = r1 - a1 * s1
        w2 = w1 - a1 * (n1 + b1 * n0)
        return r1, s1, r2, w2

    _, _, r2, w2 = second(v[0], y[0], y[1], y[2])
    reduce_start(2, r2, w2)
    ret_copy(2).start()

    locs[2].wait()
    for it in range(ITERS):
        ret_copy(it).wait_recv()
    g2, d2 = reduce_end(2)
    b2 = g2 / g1
    a2 = g2 / (d2 - b2 * g2 / a1)

    def finish(level, r0, w0, n0, n1):
        r1, s1, r2, w2 = second(r0, w0, n0, n1)
        p1 = r1 + b1 * r0
        x_out[0, level] = (a0 * r0 + a1 * p1) + a2 * (r2 + b2 * p1)
        r_out[0, level] = r2 - a2 * (w2 + b2 * s1)

    finish(lev, v[0, lev], y[0, lev], y[1, lev], y[2, lev])
    finish(other, home[...], rt[0], rt[1], rt[2])

    for s in swaps:
        s.wait_send()
    ob_copy.wait_send()
    pl.when(has_prev)(wn_copy.wait_send)
    for it in range(ITERS):
        edges_wait_send(eo, ei, h_send, h_recv, it)
        edges_wait_send(go, gi, g_send, g_recv, it)
        ret_copy(it).wait_send()
        most = red.at[it, pl.ds(0, count - 1)]
        pltpu.make_async_copy(most, most, rd_send.at[it]).wait()

        @pl.when(has_prev)
        def _():
            for k in range(many):
                back_copy(it, k).wait_send()

    @pl.when(has_next)
    def _():
        for k in range(many):
            forth_copy(ITERS - 1, k).wait_send()


def on_device(wins, tiles, right_side, error_weight, coeffs, obs_block, obs_pos, obs_weight):
    _, levels, rows, cols = right_side.shape
    nblk, width = obs_pos.shape[1:]
    f32 = jnp.float32
    vm = functools.partial(pltpu.VMEM, dtype=f32)
    dma = pltpu.SemaphoreType.DMA
    anyspace = pl.BlockSpec(memory_space=pl.ANY)
    vmem = pl.BlockSpec(memory_space=pltpu.VMEM)
    many = rows // EDGE
    scratch = [
        pltpu.VMEM(obs_block.shape, jnp.int32),
        pltpu.VMEM(obs_pos.shape, jnp.int32),
        vm(obs_weight.shape),
        vm((2, 2, rows, cols)),
        vm((ITERS, 2, rows, cols)),
        vm((2, rows, cols)),
        vm((rows, cols)),
        vm((4, 2, rows, cols)),
        vm((2, rows, cols)),
        vm((2, nblk + 8, width)),
        vm((2, rows, cols)),
        vm((ITERS, rows, cols)),
        vm((ITERS, rows, cols)),
        vm((rows, cols)),
        vm((ITERS, 2, 2, cols)),
        vm((ITERS, 2, 2, cols)),
        vm((ITERS, 2, 2, cols)),
        vm((ITERS, 2, 2, cols)),
        vm((ITERS, rows, cols)),
        vm((rows, cols)),
        vm((ITERS, 2, 128)),
        vm((ITERS, wins * tiles, 2, 128)),
        dma((3 + many,)), dma((3 + many,)), dma((7,)),
        dma((ITERS, 2)), dma((ITERS, 2)),
        dma((2, ITERS, many)), dma((2, ITERS, many)),
        dma((ITERS, 2)), dma((ITERS, 2)),
        dma((ITERS,)), dma((ITERS,)),
        dma((ITERS,)), dma((ITERS,)),
        dma, dma,
    ]
    out = jax.ShapeDtypeStruct(right_side.shape, f32)
    return pl.pallas_call(
        functools.partial(kernel, wins, tiles),
        out_shape=(out, out),
        in_specs=[anyspace] * 6,
        out_specs=(vmem, vmem),
        scratch_shapes=scratch,
        compiler_params=pltpu.CompilerParams(has_side_effects=True,
                                             vmem_limit_bytes=60 * 1024 * 1024),
    )(right_side, error_weight, coeffs, obs_block, obs_pos, obs_weight)


def solution(mesh):
    in_specs = (
        P("win", None, "tile", None),
        P("win", None, "tile", None),
        P(None, "win", None, "tile", None),
        P("win", "tile"),
        P("win", "tile", None),
        P("win", "tile", None),
    )
    out_specs = (P("win", None, "tile", None), P("win", None, "tile", None))
    return jax.shard_map(
        functools.partial(on_device, mesh.shape["win"], mesh.shape["tile"]),
        mesh=mesh, in_specs=in_specs, out_specs=out_specs, check_vma=False
    )
```
